32 devices in a mesh: ctx: 8 (over y, x, core), dp: 4 (over z).
Axes of the slice: x: 2, y: 2, z: 4, core: 2. Of those that a mesh axis runs over, the one named last changes fastest.
Arguments:
- query_previous: bfloat16 [4, 1024, 2048], P('dp', 'ctx'), may hold values from -240 to 240
- key_previous: bfloat16 [4, 1024, 512], P('dp', 'ctx'), may hold values from -6 to 6
- value_previous: bfloat16 [4, 1024, 512], P('dp', 'ctx'), may hold values from -6 to 6
- span_order: int32 [16], replicated, may hold values from 0 to 15, each once
- resid: bfloat16 [4, 1024, 4096], P('dp', 'ctx'), may hold values from -6 to 6
- grad_norm: bfloat16 [4, 1024, 4096], P('dp', 'ctx'), may hold values from -3 to 3
- gain: float32 [4096], replicated, may hold values from 0.1 to 1.9
Outputs:
- out_prev: bfloat16 [4, 1024, 2048], P('dp', 'ctx')
- lse_prev: float32 [4, 16, 1024], P('dp', None, 'ctx')
- resid_grad: bfloat16 [4, 1024, 4096], P('dp', 'ctx')
- gain_grad: float32 [4096], replicated
The draws below stay inside these ranges and needn't reach their ends.
Inputs may be any that keep to these rules, and one draw needn't show every extreme that they name: span_order names each of the 16 spans once; rows c * 64 to (c + 1) * 64 - 1 of a sequence's arrays hold span span_order[c].
All inputs are finite; a program needn't handle non-finite values.
Results may differ from the reference program's by a relative error of at most 0.0055.
Values may be sent and summed in bfloat16 or wider, within the bound.
A program may use at most 64 MiB of HBM per device.

```python
import math
import jax
import jax.numpy as jnp
from jax import lax

D = 4096
QUERY_HEADS = 16
KEY_VALUE_HEADS = 4
HEAD_WIDTH = 128
TOK_DEV = 128
SPANS = 16
SEQUENCE_TOKENS = 1024
SEQUENCE_COUNT = 4
N_CTX = 8


def draw_query_previous(key, part):
    base = jax.random.truncated_normal(key, -6.0, 6.0, (SEQUENCE_COUNT, SEQUENCE_TOKENS, QUERY_HEADS * HEAD_WIDTH), jnp.float32)
    return base.astype(jnp.bfloat16)


def block_levels(own_key, extent, split, low, top_value):
    factor_of, own = 1.0, jax.random.fold_in(own_key, 6)
    for dim, blocks in split:
        steps = jnp.exp(jax.random.uniform(jax.random.fold_in(own, dim), (blocks,), jnp.float32, low / len(split), top_value / len(split)))
        factor_of = factor_of * jnp.repeat(steps, extent[dim] // blocks).reshape([-1 if axis == dim else 1 for axis in range(len(extent))])
    return factor_of


def scatter_about(stream_key, dims, deviation, limit, cuts=(), kind=jnp.bfloat16):
    result = jax.random.normal(stream_key, dims, jnp.float32) * deviation
    if len(cuts) > 0:
        result = block_levels(stream_key, dims, cuts, -0.22, 0.18) * result
    return jnp.clip(result, min=-limit, max=limit).astype(kind)


def setup_inputs(seed: int = 0) -> dict:
    key_list = jax.random.split(jax.random.key(seed), 8)
    return {
        "query_previous": draw_query_previous(jax.random.fold_in(key_list[7], 71), 0),
        "key_previous": scatter_about(key_list[1], (SEQUENCE_COUNT, SEQUENCE_TOKENS, KEY_VALUE_HEADS * HEAD_WIDTH), 1.0, 6.0, ((0, 4), (1, 8))),
        "value_previous": scatter_about(key_list[2], (SEQUENCE_COUNT, SEQUENCE_TOKENS, KEY_VALUE_HEADS * HEAD_WIDTH), 1.0, 6.0, ((0, 4), (1, 8))),
        "span_order": jax.random.permutation(key_list[3], SPANS).astype(jnp.int32),
        "resid": scatter_about(key_list[4], (SEQUENCE_COUNT, SEQUENCE_TOKENS, D), 1.0, 6.0, ((0, 4), (1, 8))),
        "grad_norm": scatter_about(key_list[5], (SEQUENCE_COUNT, SEQUENCE_TOKENS, D), 0.5, 3.0, ((0, 4), (1, 8))),
        "gain": jnp.clip(1.0 + 0.18 * jax.random.normal(key_list[6], (D,), jnp.float32), 0.1, 1.9),
    }


def positions(span_order):
    half = TOK_DEV // 2
    index = jnp.arange(TOK_DEV * N_CTX, dtype=jnp.int32)
    return (span_order[index // half] * half + index % half).astype(jnp.int32)

def attend_rows(query_rows, q_positions, key_rows, value_rows, k_positions):
    query_group = QUERY_HEADS // KEY_VALUE_HEADS
    tally_count = query_rows.shape[0]
    query_four_axes = query_rows.astype(jnp.float32).reshape(tally_count, KEY_VALUE_HEADS, query_group, HEAD_WIDTH)
    key_three_axes = key_rows.astype(jnp.float32).reshape(-1, KEY_VALUE_HEADS, HEAD_WIDTH)
    value_three_axes = value_rows.astype(jnp.float32).reshape(-1, KEY_VALUE_HEADS, HEAD_WIDTH)
    scores = jnp.einsum('rkgd,skd->kgrs', query_four_axes, key_three_axes) * HEAD_WIDTH ** (-0.5)
    mask = (k_positions[None, :] <= q_positions[:, None])[None, None]
    scores = jnp.where(mask, scores, -1e+30)
    top = lax.optimization_barrier(jnp.max(scores, axis=-1))
    weights = jnp.where(mask, jnp.exp(scores - top[..., None]), 0.0)
    total = lax.optimization_barrier(jnp.sum(weights, axis=-1))
    probs = lax.optimization_barrier(weights.astype(jnp.bfloat16)).astype(jnp.float32)
    summed = jnp.einsum('kgrs,skd->rkgd', probs, value_three_axes)
    output = summed / jnp.transpose(total, (2, 0, 1))[..., None]
    lse = (top + jnp.log(total)).reshape(QUERY_HEADS, tally_count)
    return (output.reshape(tally_count, QUERY_HEADS * HEAD_WIDTH).astype(jnp.bfloat16), lse)

def reference(query_previous, key_previous, value_previous, span_order, resid, grad_norm, gain):
    length = TOK_DEV * N_CTX
    pos = positions(span_order)
    block = math.gcd(length, 512)
    blocks = length // block

    def one_sequence(items):
        query_rows, key_rows, value_rows = items
        q_blocks = query_rows.reshape(blocks, block, QUERY_HEADS * HEAD_WIDTH)
        p_blocks = pos.reshape(blocks, block)
        outs, lses = lax.map(lambda pair: attend_rows(pair[0], pair[1], key_rows, value_rows, pos), (q_blocks, p_blocks))
        lse = jnp.transpose(lses, (1, 0, 2)).reshape(QUERY_HEADS, length)
        return (outs.reshape(length, QUERY_HEADS * HEAD_WIDTH), lse)
    out_prev, lse_prev = lax.map(one_sequence, (query_previous, key_previous, value_previous))
    resid_f = resid.astype(jnp.float32)
    grad_f = grad_norm.astype(jnp.float32)
    inv_rms = 1.0 / jnp.sqrt(lax.optimization_barrier(jnp.mean(resid_f * resid_f, axis=-1, keepdims=True)) + 1e-05)
    normed = resid_f * inv_rms
    gain_grad = lax.optimization_barrier(jnp.sum(grad_f * normed, axis=(0, 1)))
    scaled = gain[None, None, :] * grad_f
    resid_grad = ((scaled - normed * lax.optimization_barrier(jnp.mean(scaled * normed, axis=-1, keepdims=True))) * inv_rms).astype(jnp.bfloat16)
    return (out_prev, lse_prev, resid_grad, gain_grad)
```

```python
import functools
import math

import jax
import jax.numpy as jnp
from jax import lax
from jax.experimental import pallas as pl
from jax.experimental.pallas import tpu as pltpu
from jax.sharding import PartitionSpec as P

HEAD_WIDTH = 128
MESH = pl.DeviceIdType.MESH
LOW = -1e30


def kernel(
    n,
    dp_count,
    heads,
    kv_heads,
    q_hbm,
    k_hbm,
    v_hbm,
    span_hbm,
    resid_hbm,
    grad_hbm,
    gain_hbm,
    out_hbm,
    lse_hbm,
    rgrad_hbm,
    ggrad_hbm,
    k_all,
    v_all,
    q_buf,
    q_turned,
    spans,
    resid_buf,
    grad_buf,
    gain_buf,
    tops,
    totals,
    summed,
    out_buf,
    lse_buf,
    rgrad_buf,
    terms,
    part,
    part_in,
    level,
    whole,
    ggrad_buf,
    local_sem,
    kv_send,
    kv_recv,
    p1_send,
    p1_recv,
    p2_send,
    p2_recv,
    p3_send,
    p3_recv,
):
    rows = q_hbm.shape[0]
    width = resid_hbm.shape[1]
    half = rows // 2
    group = heads // kv_heads
    chips = n // 2
    piece = width // n
    span_count = span_hbm.shape[0]
    me = lax.axis_index("ctx")
    mine_dp = lax.axis_index("dp")
    chip = me // 2
    core = me % 2
    sibling = chip * 2 + (1 - core)
    square = chips == 4

    def other_chip(k):
        if square:
            low, high = chip % 2, chip // 2
            low = 1 - low if k % 2 else low
            high = 1 - high if k // 2 else high
            return high * 2 + low
        return (chip + k) % chips

    def ctx_peer(k):
        return (me + k) % n

    def dp_peer(k):
        return (mine_dp + k) % dp_count

    barrier = pltpu.get_barrier_semaphore()
    for k in range(1, n):
        pl.semaphore_signal(barrier, inc=1, device_id={"ctx": ctx_peer(k)}, device_id_type=MESH)
    for k in range(1, dp_count):
        pl.semaphore_signal(barrier, inc=1, device_id={"dp": dp_peer(k)}, device_id_type=MESH)

    def slot(ref, index, count=1):
        return ref.at[pl.ds(pl.multiple_of(index * rows, rows), count * rows), :]

    own_k = pltpu.make_async_copy(k_hbm, slot(k_all, me), local_sem.at[0])
    own_v = pltpu.make_async_copy(v_hbm, slot(v_all, me), local_sem.at[1])
    get_resid = pltpu.make_async_copy(resid_hbm, resid_buf, local_sem.at[2])
    get_grad = pltpu.make_async_copy(grad_hbm, grad_buf, local_sem.at[3])
    get_gain = pltpu.make_async_copy(gain_hbm, gain_buf, local_sem.at[4])
    get_span = pltpu.make_async_copy(span_hbm, spans, local_sem.at[5])
    get_q = pltpu.make_async_copy(q_hbm, q_buf, local_sem.at[6])
    for copy in (own_k, own_v, get_resid, get_grad, get_gain, get_span, get_q):
        copy.start()

    k_or_v = (k_all, v_all)
    source = (k_hbm, v_hbm)
    sends = []

    def send(which, index, target, lane, first=False):
        src = source[which] if first else slot(k_or_v[which], index)
        copy = pltpu.make_async_remote_copy(
            src_ref=src,
            dst_ref=slot(k_or_v[which], index),
            send_sem=kv_send.at[which, lane],
            recv_sem=kv_recv.at[which, index],
            device_id={"ctx": target},
            device_id_type=MESH,
        )
        copy.start()
        sends.append(copy)

    def arrived(which, index):
        pltpu.make_async_remote_copy(
            src_ref=slot(k_or_v[which], index),
            dst_ref=slot(k_or_v[which], index),
            send_sem=kv_send.at[which, 0],
            recv_sem=kv_recv.at[which, index],
            device_id={"ctx": sibling},
            device_id_type=MESH,
        ).wait_recv()

    pl.semaphore_wait(barrier, n - 1 + dp_count - 1)

    if square:
        send(0, me, other_chip(1) * 2 + core, 1, True)
        send(1, me, other_chip(2) * 2 + core, 2, True)
        send(1, me, other_chip(1) * 2 + core, 1, True)
        send(0, me, other_chip(2) * 2 + core, 2, True)
    else:
        for k in range(1, chips):
            send(0, me, other_chip(k) * 2 + core, k, True)
            send(1, me, other_chip(k) * 2 + core, k, True)
    send(0, me, sibling, 0, True)
    send(1, me, sibling, 0, True)

    get_resid.wait()
    get_grad.wait()
    get_gain.wait()
    tile, cols = 16, 512
    terms[...] = jnp.zeros_like(terms)

    def norm_rows(step, carry):
        at = pl.ds(pl.multiple_of(step * tile, tile), tile)
        squares = jnp.zeros((tile, cols), jnp.float32)
        products = jnp.zeros((tile, cols), jnp.float32)
        for c in range(0, width, cols):
            r = resid_buf[at, c : c + cols].astype(jnp.float32)
            g = grad_buf[at, c : c + cols].astype(jnp.float32)
            squares = squares + r * r
            products = products + gain_buf[:, c : c + cols] * g * r
        mean_square = jnp.sum(squares, axis=1, keepdims=True) * (1.0 / width)
        inv = 1.0 / jnp.sqrt(mean_square + 1e-05)
        mean_product = jnp.sum(products, axis=1, keepdims=True) * inv * (1.0 / width)
        for c in range(0, width, cols):
            r = resid_buf[at, c : c + cols].astype(jnp.float32)
            g = grad_buf[at, c : c + cols].astype(jnp.float32)
            normed = r * inv
            term = g * normed
            terms[:, c : c + cols] += term[:8] + term[8:]
            scaled = gain_buf[:, c : c + cols] * g
            rgrad_buf[at, c : c + cols] = ((scaled - normed * mean_product) * inv).astype(
                rgrad_buf.dtype
            )
        return carry

    lax.fori_loop(0, rows // tile, norm_rows, 0)
    put_rgrad = pltpu.make_async_copy(rgrad_buf, rgrad_hbm, local_sem.at[7])
    put_rgrad.start()
    for r in range(n):
        part[r] = jnp.sum(terms[:, r * piece : (r + 1) * piece], axis=0, keepdims=True)

    get_q.wait()
    for h in range(heads):
        turned = jnp.transpose(q_buf[:, h * HEAD_WIDTH : (h + 1) * HEAD_WIDTH])
        q_turned[h // group, :, (h % group) * rows : (h % group + 1) * rows] = turned

    p1 = []
    for k in range(1, n):
        peer = ctx_peer(k)
        copy = pltpu.make_async_remote_copy(
            src_ref=part.at[peer],
            dst_ref=part_in.at[me],
            send_sem=p1_send.at[k],
            recv_sem=p1_recv.at[k],
            device_id={"ctx": peer},
            device_id_type=MESH,
        )
        copy.start()
        p1.append(copy)
    part_in[me] = part[me]

    get_span.wait()
    lane = lax.broadcasted_iota(jnp.int32, (1, rows), 1)
    q_pos = (
        jnp.where(lane < half, spans[2 * me], spans[2 * me + 1]) * half + lane % half
    )
    scale = HEAD_WIDTH ** (-0.5)
    exponent = scale * math.log2(math.e)

    def fold(other, first):
        line = lax.broadcasted_iota(jnp.int32, (2 * rows, 1), 0)
        base = jnp.full((2 * rows, 1), spans[4 * other], jnp.int32)
        for i in range(1, 4):
            base = jnp.where(line >= i * half, spans[4 * other + i], base)
        k_pos = base * half + line % half
        bias = jnp.where(k_pos <= q_pos, 0.0, LOW)
        at = pl.ds(pl.multiple_of(other * 2 * rows, 2 * rows), 2 * rows)
        for h in range(kv_heads):
            band = slice(h * HEAD_WIDTH, (h + 1) * HEAD_WIDTH)
            scores = jnp.dot(k_all[at, band], q_turned[h], preferred_element_type=jnp.float32)
            probs, factors = [], []
            for g in range(group):
                lanes = slice(g * rows, (g + 1) * rows)
                s = scores[:, lanes] + bias
                top = jnp.max(s, axis=0, keepdims=True)
                if not first:
                    before = tops[h : h + 1, lanes]
                    top = jnp.maximum(top, before)
                    factor = jnp.exp2((before - top) * exponent)
                    factors.append(factor)
                w = jnp.exp2((s - top) * exponent)
                total = jnp.sum(w, axis=0, keepdims=True)
                if not first:
                    total = total + totals[h : h + 1, lanes] * factor
                tops[h : h + 1, lanes] = top
                totals[h : h + 1, lanes] = total
                probs.append(w.astype(jnp.bfloat16))
            added = lax.dot_general(
                v_all[at, band],
                jnp.concatenate(probs, axis=1),
                (((0,), (0,)), ((), ())),
                preferred_element_type=jnp.float32,
            )
            if first:
                summed[h] = added
            else:
                summed[h] = summed[h] * jnp.concatenate(factors, axis=1) + added

    own_k.wait()
    own_v.wait()
    arrived(0, sibling)
    arrived(1, sibling)
    fold(chip, True)

    def gain_two():
        for copy in p1:
            copy.wait()
        level[mine_dp] = jnp.sum(part_in[...], axis=0)
        copies = []
        for k in range(1, dp_count):
            copy = pltpu.make_async_remote_copy(
                src_ref=level.at[mine_dp],
                dst_ref=level.at[mine_dp],
                send_sem=p2_send.at[k],
                recv_sem=p2_recv.at[k],
                device_id={"dp": dp_peer(k)},
                device_id_type=MESH,
            )
            copy.start()
            copies.append(copy)
        return copies

    def gain_three(copies):
        for copy in copies:
            copy.wait()
        whole[me] = jnp.sum(level[...], axis=0)
        copies = []
        for k in range(1, n):
            copy = pltpu.make_async_remote_copy(
                src_ref=whole.at[me],
                dst_ref=whole.at[me],
                send_sem=p3_send.at[k],
                recv_sem=p3_recv.at[k],
                device_id={"ctx": ctx_peer(k)},
                device_id_type=MESH,
            )
            copy.start()
            copies.append(copy)
        return copies

    if square:
        near, far, across = other_chip(1), other_chip(2), other_chip(3)
        near_c, far_c, across_c = near * 2 + core, far * 2 + core, across * 2 + core
        arrived(0, near_c)
        send(0, near_c, far_c, 3)
        send(0, near_c, sibling, 4)
        arrived(1, far_c)
        send(1, far_c, near_c, 3)
        send(1, far_c, sibling, 4)
        p2 = gain_two()
        arrived(1, near_c)
        send(1, near_c, sibling, 5)
        arrived(0, far_c)
        send(0, far_c, sibling, 5)
        for other in (near, far):
            arrived(0, other * 2 + 1 - core)
            arrived(1, other * 2 + 1 - core)
            fold(other, False)
        p3 = gain_three(p2)
        arrived(0, across_c)
        send(0, across_c, sibling, 6)
        arrived(1, across_c)
        send(1, across_c, sibling, 6)
        arrived(0, across * 2 + 1 - core)
        arrived(1, across * 2 + 1 - core)
        fold(across, False)
    else:
        p2 = gain_two()
        p3 = gain_three(p2)

        def step(k, carry):
            other = (chip + chips - k) % chips
            held = other * 2 + core
            for which in range(2):
                arrived(which, held)
                copy = pltpu.make_async_remote_copy(
                    src_ref=slot(k_or_v[which], held),
                    dst_ref=slot(k_or_v[which], held),
                    send_sem=kv_send.at[which, chips],
                    recv_sem=kv_recv.at[which, held],
                    device_id={"ctx": sibling},
                    device_id_type=MESH,
                )
                copy.start()
                arrived(which, other * 2 + 1 - core)
                copy.wait_send()
            fold(other, False)
            return carry

        lax.fori_loop(1, chips, step, 0)

    for h in range(heads):
        lanes = slice((h % group) * rows, (h % group + 1) * rows)
        kv = h // group
        total = totals[kv : kv + 1, lanes]
        lse_buf[h : h + 1, :] = tops[kv : kv + 1, lanes] * scale + jnp.log(total)
        out_buf[:, h * HEAD_WIDTH : (h + 1) * HEAD_WIDTH] = jnp.transpose(
            summed[kv, :, lanes] * (1.0 / total)
        ).astype(out_buf.dtype)
    put_out = pltpu.make_async_copy(out_buf, out_hbm, local_sem.at[8])
    put_out.start()
    put_lse = pltpu.make_async_copy(lse_buf, lse_hbm, local_sem.at[9])
    put_lse.start()
    for copy in p3:
        copy.wait()
    for r in range(n):
        ggrad_buf[:, r * piece : (r + 1) * piece] = whole[r]
    put_ggrad = pltpu.make_async_copy(ggrad_buf, ggrad_hbm, local_sem.at[10])
    put_ggrad.start()
    for copy in sends:
        copy.wait_send()
    for copy in (put_rgrad, put_out, put_lse, put_ggrad):
        copy.wait()


def per_device(n, dp_count, query, key, value, span_order, resid, grad_norm, gain):
    rows, q_width = query.shape[1:]
    kv_width = key.shape[2]
    width = resid.shape[2]
    heads, kv_heads = q_width // HEAD_WIDTH, kv_width // HEAD_WIDTH
    group = heads // kv_heads
    piece = width // n
    f32, bf16 = jnp.float32, jnp.bfloat16
    dma = pltpu.SemaphoreType.DMA
    lanes = max(8, n // 2 + 1)
    out, lse, rgrad, ggrad = pl.pallas_call(
        functools.partial(kernel, n, dp_count, heads, kv_heads),
        out_shape=(
            jax.ShapeDtypeStruct((rows, q_width), bf16),
            jax.ShapeDtypeStruct((heads, rows), f32),
            jax.ShapeDtypeStruct((rows, width), bf16),
            jax.ShapeDtypeStruct((1, width), f32),
        ),
        in_specs=[pl.BlockSpec(memory_space=pl.ANY)] * 7,
        out_specs=[pl.BlockSpec(memory_space=pl.ANY)] * 4,
        scratch_shapes=[
            pltpu.VMEM((n * rows, kv_width), bf16),
            pltpu.VMEM((n * rows, kv_width), bf16),
            pltpu.VMEM((rows, q_width), bf16),
            pltpu.VMEM((kv_heads, HEAD_WIDTH, group * rows), bf16),
            pltpu.SMEM(span_order.shape, jnp.int32),
            pltpu.VMEM((rows, width), bf16),
            pltpu.VMEM((rows, width), bf16),
            pltpu.VMEM((1, width), f32),
            pltpu.VMEM((kv_heads, group * rows), f32),
            pltpu.VMEM((kv_heads, group * rows), f32),
            pltpu.VMEM((kv_heads, HEAD_WIDTH, group * rows), f32),
            pltpu.VMEM((rows, q_width), bf16),
            pltpu.VMEM((heads, rows), f32),
            pltpu.VMEM((rows, width), bf16),
            pltpu.VMEM((8, width), f32),
            pltpu.VMEM((n, 1, piece), f32),
            pltpu.VMEM((n, 1, piece), f32),
            pltpu.VMEM((dp_count, 1, piece), f32),
            pltpu.VMEM((n, 1, piece), f32),
            pltpu.VMEM((1, width), f32),
            dma((11,)),
            dma((2, lanes)),
            dma((2, n)),
            dma((n,)),
            dma((n,)),
            dma((dp_count,)),
            dma((dp_count,)),
            dma((n,)),
            dma((n,)),
        ],
        compiler_params=pltpu.CompilerParams(collective_id=0, has_side_effects=True),
    )(
        query[0],
        key[0],
        value[0],
        span_order,
        resid[0],
        grad_norm[0],
        gain[None, :],
    )
    return (out[None], lse[None], rgrad[None], ggrad[0])


def solution(mesh):
    return jax.shard_map(
        functools.partial(per_device, mesh.shape["ctx"], mesh.shape["dp"]),
        mesh=mesh,
        in_specs=(
            P("dp", "ctx", None),
            P("dp", "ctx", None),
            P("dp", "ctx", None),
            P(),
            P("dp", "ctx", None),
            P("dp", "ctx", None),
            P(),
        ),
        out_specs=(P("dp", "ctx", None), P("dp", None, "ctx"), P("dp", "ctx", None), P()),
        check_vma=False,
    )
```

```python
import functools
import math

import jax
import jax.numpy as jnp
from jax import lax
from jax.experimental import pallas as pl
from jax.experimental.pallas import tpu as pltpu
from jax.sharding import PartitionSpec as P

HEAD_WIDTH = 128
MESH = pl.DeviceIdType.MESH
LOW = -1e30


def kernel(
    n,
    dp_count,
    heads,
    kv_heads,
    q_hbm,
    k_hbm,
    v_hbm,
    span_hbm,
    resid_hbm,
    grad_hbm,
    gain_hbm,
    summed,
    tops,
    totals,
    rgrad_buf,
    ggrad_buf,
    k_all,
    v_all,
    q_buf,
    q_turned,
    spans,
    resid_buf,
    grad_buf,
    gain_buf,
    terms,
    part,
    part_in,
    level,
    whole,
    local_sem,
    kv_send,
    kv_recv,
    p1_send,
    p1_recv,
    p2_send,
    p2_recv,
    p3_send,
    p3_recv,
):
    rows = q_hbm.shape[0]
    width = resid_hbm.shape[1]
    half = rows // 2
    group = heads // kv_heads
    chips = n // 2
    piece = width // n
    span_count = span_hbm.shape[0]
    me = lax.axis_index("ctx")
    mine_dp = lax.axis_index("dp")
    chip = me // 2
    core = me % 2
    sibling = chip * 2 + (1 - core)
    square = chips == 4

    def other_chip(k):
        if square:
            low, high = chip % 2, chip // 2
            low = 1 - low if k % 2 else low
            high = 1 - high if k // 2 else high
            return high * 2 + low
        return (chip + k) % chips

    def ctx_peer(k):
        return (me + k) % n

    def dp_peer(k):
        return (mine_dp + k) % dp_count

    barrier = pltpu.get_barrier_semaphore()
    for k in range(1, n):
        pl.semaphore_signal(barrier, inc=1, device_id={"ctx": ctx_peer(k)}, device_id_type=MESH)
    for k in range(1, dp_count):
        pl.semaphore_signal(barrier, inc=1, device_id={"dp": dp_peer(k)}, device_id_type=MESH)

    def slot(ref, index, count=1):
        return ref.at[pl.ds(pl.multiple_of(index * rows, rows), count * rows), :]

    own_k = pltpu.make_async_copy(k_hbm, slot(k_all, me), local_sem.at[0])
    own_v = pltpu.make_async_copy(v_hbm, slot(v_all, me), local_sem.at[1])
    get_resid = pltpu.make_async_copy(resid_hbm, resid_buf, local_sem.at[2])
    get_grad = pltpu.make_async_copy(grad_hbm, grad_buf, local_sem.at[3])
    get_gain = pltpu.make_async_copy(gain_hbm, gain_buf, local_sem.at[4])
    get_span = pltpu.make_async_copy(span_hbm, spans, local_sem.at[5])
    get_q = pltpu.make_async_copy(q_hbm, q_buf, local_sem.at[6])
    for copy in (own_k, own_v, get_resid, get_grad, get_gain, get_span, get_q):
        copy.start()

    k_or_v = (k_all, v_all)
    source = (k_hbm, v_hbm)
    sends = []

    def send(which, index, target, lane, first=False):
        src = source[which] if first else slot(k_or_v[which], index)
        copy = pltpu.make_async_remote_copy(
            src_ref=src,
            dst_ref=slot(k_or_v[which], index),
            send_sem=kv_send.at[which, lane],
            recv_sem=kv_recv.at[which, index],
            device_id={"ctx": target},
            device_id_type=MESH,
        )
        copy.start()
        sends.append(copy)

    def arrived(which, index):
        pltpu.make_async_remote_copy(
            src_ref=slot(k_or_v[which], index),
            dst_ref=slot(k_or_v[which], index),
            send_sem=kv_send.at[which, 0],
            recv_sem=kv_recv.at[which, index],
            device_id={"ctx": sibling},
            device_id_type=MESH,
        ).wait_recv()

    pl.semaphore_wait(barrier, n - 1 + dp_count - 1)

    if square:
        send(0, me, other_chip(1) * 2 + core, 1, True)
        send(1, me, other_chip(2) * 2 + core, 2, True)
        send(1, me, other_chip(1) * 2 + core, 1, True)
        send(0, me, other_chip(2) * 2 + core, 2, True)
    else:
        for k in range(1, chips):
            send(0, me, other_chip(k) * 2 + core, k, True)
            send(1, me, other_chip(k) * 2 + core, k, True)
    send(0, me, sibling, 0, True)
    send(1, me, sibling, 0, True)

    get_resid.wait()
    get_grad.wait()
    get_gain.wait()
    tile, cols = 16, 512
    terms[...] = jnp.zeros_like(terms)

    def norm_rows(step, carry):
        at = pl.ds(pl.multiple_of(step * tile, tile), tile)
        squares = jnp.zeros((tile, cols), jnp.float32)
        products = jnp.zeros((tile, cols), jnp.float32)
        for c in range(0, width, cols):
            r = resid_buf[at, c : c + cols].astype(jnp.float32)
            g = grad_buf[at, c : c + cols].astype(jnp.float32)
            squares = squares + r * r
            products = products + gain_buf[:, c : c + cols] * g * r
        mean_square = jnp.sum(squares, axis=1, keepdims=True) * (1.0 / width)
        inv = 1.0 / jnp.sqrt(mean_square + 1e-05)
        mean_product = jnp.sum(products, axis=1, keepdims=True) * inv * (1.0 / width)
        for c in range(0, width, cols):
            r = resid_buf[at, c : c + cols].astype(jnp.float32)
            g = grad_buf[at, c : c + cols].astype(jnp.float32)
            normed = r * inv
            term = g * normed
            terms[:, c : c + cols] += term[:8] + term[8:]
            scaled = gain_buf[:, c : c + cols] * g
            rgrad_buf[at, c : c + cols] = ((scaled - normed * mean_product) * inv).astype(
                rgrad_buf.dtype
            )
        return carry

    lax.fori_loop(0, rows // tile, norm_rows, 0)
    for r in range(n):
        part[r] = jnp.sum(terms[:, r * piece : (r + 1) * piece], axis=0, keepdims=True)

    get_q.wait()
    for h in range(heads):
        turned = jnp.transpose(q_buf[:, h * HEAD_WIDTH : (h + 1) * HEAD_WIDTH])
        q_turned[h // group, :, (h % group) * rows : (h % group + 1) * rows] = turned

    p1 = []
    for k in range(1, n):
        peer = ctx_peer(k)
        copy = pltpu.make_async_remote_copy(
            src_ref=part.at[peer],
            dst_ref=part_in.at[me],
            send_sem=p1_send.at[k],
            recv_sem=p1_recv.at[k],
            device_id={"ctx": peer},
            device_id_type=MESH,
        )
        copy.start()
        p1.append(copy)
    part_in[me] = part[me]

    get_span.wait()
    lane = lax.broadcasted_iota(jnp.int32, (1, rows), 1)
    q_pos = (
        jnp.where(lane < half, spans[2 * me], spans[2 * me + 1]) * half + lane % half
    )
    scale = HEAD_WIDTH ** (-0.5)
    exponent = scale * math.log2(math.e)

    def fold(other, first):
        line = lax.broadcasted_iota(jnp.int32, (2 * rows, 1), 0)
        base = jnp.full((2 * rows, 1), spans[4 * other], jnp.int32)
        for i in range(1, 4):
            base = jnp.where(line >= i * half, spans[4 * other + i], base)
        k_pos = base * half + line % half
        bias = jnp.where(k_pos <= q_pos, 0.0, LOW)
        at = pl.ds(pl.multiple_of(other * 2 * rows, 2 * rows), 2 * rows)
        for h in range(kv_heads):
            band = slice(h * HEAD_WIDTH, (h + 1) * HEAD_WIDTH)
            scores = jnp.dot(k_all[at, band], q_turned[h], preferred_element_type=jnp.float32)
            probs, factors = [], []
            for g in range(group):
                lanes = slice(g * rows, (g + 1) * rows)
                s = scores[:, lanes] + bias
                top = jnp.max(s, axis=0, keepdims=True)
                if not first:
                    before = tops[h : h + 1, lanes]
                    top = jnp.maximum(top, before)
                    factor = jnp.exp2((before - top) * exponent)
                    factors.append(factor)
                w = jnp.exp2((s - top) * exponent)
                total = jnp.sum(w, axis=0, keepdims=True)
                if not first:
                    total = total + totals[h : h + 1, lanes] * factor
                tops[h : h + 1, lanes] = top
                totals[h : h + 1, lanes] = total
                probs.append(w.astype(jnp.bfloat16))
            added = lax.dot_general(
                v_all[at, band],
                jnp.concatenate(probs, axis=1),
                (((0,), (0,)), ((), ())),
                preferred_element_type=jnp.float32,
            )
            if first:
                summed[h] = added
            else:
                summed[h] = summed[h] * jnp.concatenate(factors, axis=1) + added

    own_k.wait()
    own_v.wait()
    arrived(0, sibling)
    arrived(1, sibling)
    fold(chip, True)

    def gain_two():
        for copy in p1:
            copy.wait()
        level[mine_dp] = jnp.sum(part_in[...], axis=0)
        copies = []
        for k in range(1, dp_count):
            copy = pltpu.make_async_remote_copy(
                src_ref=level.at[mine_dp],
                dst_ref=level.at[mine_dp],
                send_sem=p2_send.at[k],
                recv_sem=p2_recv.at[k],
                device_id={"dp": dp_peer(k)},
                device_id_type=MESH,
            )
            copy.start()
            copies.append(copy)
        return copies

    def gain_three(copies):
        for copy in copies:
            copy.wait()
        whole[me] = jnp.sum(level[...], axis=0)
        copies = []
        for k in range(1, n):
            copy = pltpu.make_async_remote_copy(
                src_ref=whole.at[me],
                dst_ref=whole.at[me],
                send_sem=p3_send.at[k],
                recv_sem=p3_recv.at[k],
                device_id={"ctx": ctx_peer(k)},
                device_id_type=MESH,
            )
            copy.start()
            copies.append(copy)
        return copies

    if square:
        near, far, across = other_chip(1), other_chip(2), other_chip(3)
        near_c, far_c, across_c = near * 2 + core, far * 2 + core, across * 2 + core
        arrived(0, near_c)
        send(0, near_c, far_c, 3)
        send(0, near_c, sibling, 4)
        arrived(1, far_c)
        send(1, far_c, near_c, 3)
        send(1, far_c, sibling, 4)
        p2 = gain_two()
        arrived(1, near_c)
        send(1, near_c, sibling, 5)
        arrived(0, far_c)
        send(0, far_c, sibling, 5)
        for other in (near, far):
            arrived(0, other * 2 + 1 - core)
            arrived(1, other * 2 + 1 - core)
            fold(other, False)
        p3 = gain_three(p2)
        arrived(0, across_c)
        send(0, across_c, sibling, 6)
        arrived(1, across_c)
        send(1, across_c, sibling, 6)
        arrived(0, across * 2 + 1 - core)
        arrived(1, across * 2 + 1 - core)
        fold(across, False)
    else:
        p2 = gain_two()
        p3 = gain_three(p2)

        def step(k, carry):
            other = (chip + chips - k) % chips
            held = other * 2 + core
            for which in range(2):
                arrived(which, held)
                copy = pltpu.make_async_remote_copy(
                    src_ref=slot(k_or_v[which], held),
                    dst_ref=slot(k_or_v[which], held),
                    send_sem=kv_send.at[which, chips],
                    recv_sem=kv_recv.at[which, held],
                    device_id={"ctx": sibling},
                    device_id_type=MESH,
                )
                copy.start()
                arrived(which, other * 2 + 1 - core)
                copy.wait_send()
            fold(other, False)
            return carry

        lax.fori_loop(1, chips, step, 0)

    for copy in p3:
        copy.wait()
    for r in range(n):
        ggrad_buf[:, r * piece : (r + 1) * piece] = whole[r]
    for copy in sends:
        copy.wait_send()

def finish(
    heads, kv_heads, summed, tops, totals, rgrad, ggrad,
    out_hbm, lse_hbm, rgrad_hbm, ggrad_hbm, out_buf, lse_buf, sem
):
    rows = out_hbm.shape[0]
    group = heads // kv_heads
    scale = HEAD_WIDTH ** (-0.5)
    puts = [
        pltpu.make_async_copy(rgrad, rgrad_hbm, sem.at[0]),
        pltpu.make_async_copy(ggrad, ggrad_hbm, sem.at[1]),
    ]
    for copy in puts:
        copy.start()
    for kv in range(kv_heads):
        for g in range(group):
            h = kv * group + g
            lanes = slice(g * rows, (g + 1) * rows)
            total = totals[kv : kv + 1, lanes]
            lse_buf[h : h + 1, :] = tops[kv : kv + 1, lanes] * scale + jnp.log(total)
            out_buf[:, h * HEAD_WIDTH : (h + 1) * HEAD_WIDTH] = jnp.transpose(
                summed[kv, :, lanes] * (1.0 / total)
            ).astype(out_buf.dtype)
        band = pl.ds(kv * group * HEAD_WIDTH, group * HEAD_WIDTH)
        copy = pltpu.make_async_copy(out_buf.at[:, band], out_hbm.at[:, band], sem.at[3 + kv])
        copy.start()
        puts.append(copy)
    copy = pltpu.make_async_copy(lse_buf, lse_hbm, sem.at[2])
    copy.start()
    puts.append(copy)
    for copy in puts:
        copy.wait()


def per_device(n, dp_count, query, key, value, span_order, resid, grad_norm, gain):
    rows, q_width = query.shape[1:]
    kv_width = key.shape[2]
    width = resid.shape[2]
    heads, kv_heads = q_width // HEAD_WIDTH, kv_width // HEAD_WIDTH
    group = heads // kv_heads
    piece = width // n
    f32, bf16 = jnp.float32, jnp.bfloat16
    dma = pltpu.SemaphoreType.DMA
    lanes = max(8, n // 2 + 1)
    middle = (
        pltpu.VMEM((kv_heads, HEAD_WIDTH, group * rows), f32),
        pltpu.VMEM((kv_heads, group * rows), f32),
        pltpu.VMEM((kv_heads, group * rows), f32),
        pltpu.VMEM((rows, width), bf16),
        pltpu.VMEM((1, width), f32),
    )
    vmem = pl.BlockSpec(memory_space=pltpu.VMEM)
    results = pl.pallas_call(
        functools.partial(kernel, n, dp_count, heads, kv_heads),
        out_shape=middle,
        in_specs=[pl.BlockSpec(memory_space=pl.ANY)] * 7,
        out_specs=[vmem] * 5,
        scratch_shapes=[
            pltpu.VMEM((n * rows, kv_width), bf16),
            pltpu.VMEM((n * rows, kv_width), bf16),
            pltpu.VMEM((rows, q_width), bf16),
            pltpu.VMEM((kv_heads, HEAD_WIDTH, group * rows), bf16),
            pltpu.SMEM(span_order.shape, jnp.int32),
            pltpu.VMEM((rows, width), bf16),
            pltpu.VMEM((rows, width), bf16),
            pltpu.VMEM((1, width), f32),
            pltpu.VMEM((8, width), f32),
            pltpu.VMEM((n, 1, piece), f32),
            pltpu.VMEM((n, 1, piece), f32),
            pltpu.VMEM((dp_count, 1, piece), f32),
            pltpu.VMEM((n, 1, piece), f32),
            dma((7,)),
            dma((2, lanes)),
            dma((2, n)),
            dma((n,)),
            dma((n,)),
            dma((dp_count,)),
            dma((dp_count,)),
            dma((n,)),
            dma((n,)),
        ],
        compiler_params=pltpu.CompilerParams(collective_id=0, has_side_effects=True),
    )(
        query[0],
        key[0],
        value[0],
        span_order,
        resid[0],
        grad_norm[0],
        gain[None, :],
    )
    out, lse, rgrad, ggrad = pl.pallas_call(
        functools.partial(finish, heads, kv_heads),
        out_shape=(
            jax.ShapeDtypeStruct((rows, q_width), bf16),
            jax.ShapeDtypeStruct((heads, rows), f32),
            jax.ShapeDtypeStruct((rows, width), bf16),
            jax.ShapeDtypeStruct((1, width), f32),
        ),
        in_specs=[vmem] * 5,
        out_specs=[pl.BlockSpec(memory_space=pl.ANY)] * 4,
        scratch_shapes=[
            pltpu.VMEM((rows, q_width), bf16),
            pltpu.VMEM((heads, rows), f32),
            dma((3 + kv_heads,)),
        ],
    )(*(pltpu.with_memory_space_constraint(part, pltpu.VMEM) for part in results))
    return (out[None], lse[None], rgrad[None], ggrad[0])


def solution(mesh):
    return jax.shard_map(
        functools.partial(per_device, mesh.shape["ctx"], mesh.shape["dp"]),
        mesh=mesh,
        in_specs=(
            P("dp", "ctx", None),
            P("dp", "ctx", None),
            P("dp", "ctx", None),
            P(),
            P("dp", "ctx", None),
            P("dp", "ctx", None),
            P(),
        ),
        out_specs=(P("dp", "ctx", None), P("dp", None, "ctx"), P("dp", "ctx", None), P()),
        check_vma=False,
    )
```

```python
import functools
import math

import jax
import jax.numpy as jnp
from jax import lax
from jax.experimental import pallas as pl
from jax.experimental.pallas import tpu as pltpu
from jax.sharding import PartitionSpec as P

HEAD_WIDTH = 128
MESH = pl.DeviceIdType.MESH
LOW = -1e30


def kernel(
    n,
    dp_count,
    heads,
    kv_heads,
    q_hbm,
    k_hbm,
    v_hbm,
    span_hbm,
    resid_hbm,
    grad_hbm,
    gain_hbm,
    summed,
    tops,
    totals,
    rgrad_buf,
    ggrad_buf,
    k_all,
    v_all,
    q_buf,
    q_turned,
    spans,
    resid_buf,
    grad_buf,
    gain_buf,
    terms,
    part,
    part_in,
    level,
    cross,
    whole,
    local_sem,
    kv_send,
    kv_recv,
    p1_send,
    p1_recv,
    p2_send,
    p2_recv,
    p3_send,
    p3_recv,
):
    rows = q_hbm.shape[0]
    width = resid_hbm.shape[1]
    span = rows // 2
    group = heads // kv_heads
    chips = n // 2
    piece = width // 2
    pair_heads = kv_heads // 2
    cut = pair_heads * HEAD_WIDTH
    me = lax.axis_index("ctx")
    mine_dp = lax.axis_index("dp")
    chip = me // 2
    core = me % 2
    sibling = chip * 2 + (1 - core)
    square = chips == 4

    def other_chip(k):
        if square:
            low, high = chip % 2, chip // 2
            low = 1 - low if k % 2 else low
            high = 1 - high if k // 2 else high
            return high * 2 + low
        return (chip + k) % chips

    def dp_peer(k):
        return (mine_dp + k) % dp_count

    barrier = pltpu.get_barrier_semaphore()
    pl.semaphore_signal(barrier, inc=1, device_id={"ctx": sibling}, device_id_type=MESH)
    for k in range(1, chips):
        peer = other_chip(k) * 2 + core
        pl.semaphore_signal(barrier, inc=1, device_id={"ctx": peer}, device_id_type=MESH)
    for k in range(1, dp_count):
        pl.semaphore_signal(barrier, inc=1, device_id={"dp": dp_peer(k)}, device_id_type=MESH)

    def slot(ref, index, count=1):
        return ref.at[pl.ds(pl.multiple_of(index * rows, rows), count * rows), :]

    own_k = pltpu.make_async_copy(k_hbm, slot(k_all, me), local_sem.at[0])
    own_v = pltpu.make_async_copy(v_hbm, slot(v_all, me), local_sem.at[1])
    get_resid = pltpu.make_async_copy(resid_hbm, resid_buf, local_sem.at[2])
    get_grad = pltpu.make_async_copy(grad_hbm, grad_buf, local_sem.at[3])
    get_gain = pltpu.make_async_copy(gain_hbm, gain_buf, local_sem.at[4])
    get_span = pltpu.make_async_copy(span_hbm, spans, local_sem.at[5])
    get_q = pltpu.make_async_copy(q_hbm, q_buf, local_sem.at[6])
    for copy in (own_k, own_v, get_resid, get_grad, get_gain, get_span, get_q):
        copy.start()

    k_or_v = (k_all, v_all)
    source = (k_hbm, v_hbm)
    sends = []

    def part_of(ref, half, index):
        at = pl.ds(pl.multiple_of(index * rows, rows), rows)
        return ref.at[at, half * cut : (half + 1) * cut]

    def carry(which, half, index, target, lane, first=False):
        held = part_of(k_or_v[which], half, index)
        return pltpu.make_async_remote_copy(
            src_ref=source[which].at[:, half * cut : (half + 1) * cut] if first else held,
            dst_ref=held,
            send_sem=kv_send.at[which, half, lane],
            recv_sem=kv_recv.at[which, half, index],
            device_id={"ctx": target},
            device_id_type=MESH,
        )

    def send(half, index, target, lane, first=False):
        for which in range(2):
            copy = carry(which, half, index, target, lane, first)
            copy.start()
            sends.append(copy)

    def arrived(half, index):
        for which in range(2):
            carry(which, half, index, sibling, 0).wait_recv()

    pl.semaphore_wait(barrier, chips + dp_count - 1)

    if square:
        send(0, me, other_chip(1) * 2 + core, 1, True)
        send(1, me, other_chip(2) * 2 + core, 2, True)
        send(1, me, other_chip(1) * 2 + core, 1, True)
        send(0, me, other_chip(2) * 2 + core, 2, True)
    else:
        for k in range(1, chips):
            for half in range(2):
                send(half, me, other_chip(k) * 2 + core, k, True)
    for half in range(2):
        send(half, me, sibling, 0, True)

    get_resid.wait()
    get_grad.wait()
    get_gain.wait()
    tile, cols = 16, 512
    terms[...] = jnp.zeros_like(terms)

    def norm_rows(step, carry):
        at = pl.ds(pl.multiple_of(step * tile, tile), tile)
        squares = jnp.zeros((tile, cols), jnp.float32)
        products = jnp.zeros((tile, cols), jnp.float32)
        for c in range(0, width, cols):
            r = resid_buf[at, c : c + cols].astype(jnp.float32)
            g = grad_buf[at, c : c + cols].astype(jnp.float32)
            squares = squares + r * r
            products = products + gain_buf[:, c : c + cols] * g * r
        mean_square = jnp.sum(squares, axis=1, keepdims=True) * (1.0 / width)
        inv = 1.0 / jnp.sqrt(mean_square + 1e-05)
        mean_product = jnp.sum(products, axis=1, keepdims=True) * inv * (1.0 / width)
        for c in range(0, width, cols):
            r = resid_buf[at, c : c + cols].astype(jnp.float32)
            g = grad_buf[at, c : c + cols].astype(jnp.float32)
            normed = r * inv
            term = g * normed
            terms[:, c : c + cols] += term[:8] + term[8:]
            scaled = gain_buf[:, c : c + cols] * g
            rgrad_buf[at, c : c + cols] = ((scaled - normed * mean_product) * inv).astype(
                rgrad_buf.dtype
            )
        return carry

    lax.fori_loop(0, rows // tile, norm_rows, 0)
    for r in range(2):
        part[r] = jnp.sum(terms[:, r * piece : (r + 1) * piece], axis=0, keepdims=True)

    join = pltpu.make_async_remote_copy(
        src_ref=part.at[1 - core],
        dst_ref=part_in.at[0],
        send_sem=p1_send.at[0],
        recv_sem=p1_recv.at[0],
        device_id={"ctx": sibling},
        device_id_type=MESH,
    )
    join.start()

    get_q.wait()
    for h in range(heads):
        turned = jnp.transpose(q_buf[:, h * HEAD_WIDTH : (h + 1) * HEAD_WIDTH])
        q_turned[h // group, :, (h % group) * rows : (h % group + 1) * rows] = turned

    join.wait()
    level[mine_dp] = part[core] + part_in[0]
    over_dp = []
    for k in range(1, dp_count):
        copy = pltpu.make_async_remote_copy(
            src_ref=level.at[mine_dp],
            dst_ref=level.at[mine_dp],
            send_sem=p2_send.at[k],
            recv_sem=p2_recv.at[k],
            device_id={"dp": dp_peer(k)},
            device_id_type=MESH,
        )
        copy.start()
        over_dp.append(copy)

    get_span.wait()
    lane = lax.broadcasted_iota(jnp.int32, (1, rows), 1)
    q_pos = (
        jnp.where(lane < span, spans[2 * me], spans[2 * me + 1]) * span + lane % span
    )
    scale = HEAD_WIDTH ** (-0.5)
    exponent = scale * math.log2(math.e)

    def fold(index, count, half, first=False):
        line = lax.broadcasted_iota(jnp.int32, (count * rows, 1), 0)
        base = jnp.full((count * rows, 1), spans[2 * index], jnp.int32)
        for i in range(1, 2 * count):
            base = jnp.where(line >= i * span, spans[2 * index + i], base)
        k_pos = base * span + line % span
        bias = jnp.where(k_pos <= q_pos, 0.0, LOW)
        at = pl.ds(pl.multiple_of(index * rows, rows), count * rows)
        for h in range(half * pair_heads, (half + 1) * pair_heads):
            band = slice(h * HEAD_WIDTH, (h + 1) * HEAD_WIDTH)
            scores = jnp.dot(k_all[at, band], q_turned[h], preferred_element_type=jnp.float32)
            probs, factors = [], []
            for g in range(group):
                lanes = slice(g * rows, (g + 1) * rows)
                s = scores[:, lanes] + bias
                top = jnp.max(s, axis=0, keepdims=True)
                if not first:
                    before = tops[h : h + 1, lanes]
                    top = jnp.maximum(top, before)
                    factor = jnp.exp2((before - top) * exponent)
                    factors.append(factor)
                w = jnp.exp2((s - top) * exponent)
                total = jnp.sum(w, axis=0, keepdims=True)
                if not first:
                    total = total + totals[h : h + 1, lanes] * factor
                tops[h : h + 1, lanes] = top
                totals[h : h + 1, lanes] = total
                probs.append(w.astype(jnp.bfloat16))
            added = lax.dot_general(
                v_all[at, band],
                jnp.concatenate(probs, axis=1),
                (((0,), (0,)), ((), ())),
                preferred_element_type=jnp.float32,
            )
            if first:
                summed[h] = added
            else:
                summed[h] = summed[h] * jnp.concatenate(factors, axis=1) + added

    own_k.wait()
    own_v.wait()
    for half in range(2):
        arrived(half, sibling)
        fold(chip * 2, 2, half, True)

    def gain_chips():
        for copy in over_dp:
            copy.wait()
        cross[chip] = jnp.sum(level[...], axis=0)
        copies = []
        for k in range(1, chips):
            copy = pltpu.make_async_remote_copy(
                src_ref=cross.at[chip],
                dst_ref=cross.at[chip],
                send_sem=p3_send.at[k],
                recv_sem=p3_recv.at[k],
                device_id={"ctx": other_chip(k) * 2 + core},
                device_id_type=MESH,
            )
            copy.start()
            copies.append(copy)
        return copies

    def gain_whole(copies):
        for copy in copies:
            copy.wait()
        whole[core] = jnp.sum(cross[...], axis=0)
        copy = pltpu.make_async_remote_copy(
            src_ref=whole.at[core],
            dst_ref=whole.at[core],
            send_sem=p1_send.at[1],
            recv_sem=p1_recv.at[1],
            device_id={"ctx": sibling},
            device_id_type=MESH,
        )
        copy.start()
        return copy

    if square:
        near, far, across = other_chip(1), other_chip(2), other_chip(3)
        near_c, far_c, across_c = near * 2 + core, far * 2 + core, across * 2 + core
        arrived(0, near_c)
        send(0, near_c, far_c, 3)
        send(0, near_c, sibling, 4)
        arrived(1, far_c)
        send(1, far_c, near_c, 3)
        send(1, far_c, sibling, 4)
        over_chips = gain_chips()
        arrived(0, near * 2 + 1 - core)
        fold(near * 2, 2, 0)
        arrived(1, far * 2 + 1 - core)
        fold(far * 2, 2, 1)
        arrived(1, near_c)
        send(1, near_c, sibling, 5)
        arrived(0, far_c)
        send(0, far_c, sibling, 5)
        arrived(1, near * 2 + 1 - core)
        fold(near * 2, 2, 1)
        arrived(0, far * 2 + 1 - core)
        fold(far * 2, 2, 0)
        for half in range(2):
            arrived(half, across_c)
            send(half, across_c, sibling, 6)
        for half in range(2):
            fold(across_c, 1, half)
        last = gain_whole(over_chips)
        for half in range(2):
            arrived(half, across * 2 + 1 - core)
            fold(across * 2 + 1 - core, 1, half)
    else:
        over_chips = gain_chips()

        def step(k, unused):
            other = (chip + chips - k) % chips
            held = other * 2 + core
            copies = []
            for half in range(2):
                arrived(half, held)
                for which in range(2):
                    copy = carry(which, half, held, sibling, chips)
                    copy.start()
                    copies.append(copy)
            for half in range(2):
                arrived(half, other * 2 + 1 - core)
                fold(other * 2, 2, half)
            for copy in copies:
                copy.wait_send()
            return unused

        lax.fori_loop(1, chips, step, 0)
        last = gain_whole(over_chips)

    last.wait()
    for r in range(2):
        ggrad_buf[:, r * piece : (r + 1) * piece] = whole[r]
    for copy in sends:
        copy.wait_send()

def finish(
    heads, kv_heads, summed, tops, totals, rgrad, ggrad,
    out_hbm, lse_hbm, rgrad_hbm, ggrad_hbm, out_buf, lse_buf, sem
):
    rows = out_hbm.shape[0]
    group = heads // kv_heads
    scale = HEAD_WIDTH ** (-0.5)
    puts = [
        pltpu.make_async_copy(rgrad, rgrad_hbm, sem.at[0]),
        pltpu.make_async_copy(ggrad, ggrad_hbm, sem.at[1]),
    ]
    for copy in puts:
        copy.start()
    for kv in range(kv_heads):
        for g in range(group):
            h = kv * group + g
            lanes = slice(g * rows, (g + 1) * rows)
            total = totals[kv : kv + 1, lanes]
            lse_buf[h : h + 1, :] = tops[kv : kv + 1, lanes] * scale + jnp.log(total)
            out_buf[:, h * HEAD_WIDTH : (h + 1) * HEAD_WIDTH] = jnp.transpose(
                summed[kv, :, lanes] * (1.0 / total)
            ).astype(out_buf.dtype)
        band = pl.ds(kv * group * HEAD_WIDTH, group * HEAD_WIDTH)
        copy = pltpu.make_async_copy(out_buf.at[:, band], out_hbm.at[:, band], sem.at[3 + kv])
        copy.start()
        puts.append(copy)
    copy = pltpu.make_async_copy(lse_buf, lse_hbm, sem.at[2])
    copy.start()
    puts.append(copy)
    for copy in puts:
        copy.wait()


def per_device(n, dp_count, query, key, value, span_order, resid, grad_norm, gain):
    rows, q_width = query.shape[1:]
    kv_width = key.shape[2]
    width = resid.shape[2]
    heads, kv_heads = q_width // HEAD_WIDTH, kv_width // HEAD_WIDTH
    group = heads // kv_heads
    piece = width // 2
    f32, bf16 = jnp.float32, jnp.bfloat16
    dma = pltpu.SemaphoreType.DMA
    lanes = max(8, n // 2 + 1)
    middle = (
        pltpu.VMEM((kv_heads, HEAD_WIDTH, group * rows), f32),
        pltpu.VMEM((kv_heads, group * rows), f32),
        pltpu.VMEM((kv_heads, group * rows), f32),
        pltpu.VMEM((rows, width), bf16),
        pltpu.VMEM((1, width), f32),
    )
    vmem = pl.BlockSpec(memory_space=pltpu.VMEM)
    results = pl.pallas_call(
        functools.partial(kernel, n, dp_count, heads, kv_heads),
        out_shape=middle,
        in_specs=[pl.BlockSpec(memory_space=pl.ANY)] * 7,
        out_specs=[vmem] * 5,
        scratch_shapes=[
            pltpu.VMEM((n * rows, kv_width), bf16),
            pltpu.VMEM((n * rows, kv_width), bf16),
            pltpu.VMEM((rows, q_width), bf16),
            pltpu.VMEM((kv_heads, HEAD_WIDTH, group * rows), bf16),
            pltpu.SMEM(span_order.shape, jnp.int32),
            pltpu.VMEM((rows, width), bf16),
            pltpu.VMEM((rows, width), bf16),
            pltpu.VMEM((1, width), f32),
            pltpu.VMEM((8, width), f32),
            pltpu.VMEM((2, 1, piece), f32),
            pltpu.VMEM((1, 1, piece), f32),
            pltpu.VMEM((dp_count, 1, piece), f32),
            pltpu.VMEM((n // 2, 1, piece), f32),
            pltpu.VMEM((2, 1, piece), f32),
            dma((7,)),
            dma((2, 2, lanes)),
            dma((2, 2, n)),
            dma((2,)),
            dma((2,)),
            dma((dp_count,)),
            dma((dp_count,)),
            dma((n // 2,)),
            dma((n // 2,)),
        ],
        compiler_params=pltpu.CompilerParams(collective_id=0, has_side_effects=True),
    )(
        query[0],
        key[0],
        value[0],
        span_order,
        resid[0],
        grad_norm[0],
        gain[None, :],
    )
    out, lse, rgrad, ggrad = pl.pallas_call(
        functools.partial(finish, heads, kv_heads),
        out_shape=(
            jax.ShapeDtypeStruct((rows, q_width), bf16),
            jax.ShapeDtypeStruct((heads, rows), f32),
            jax.ShapeDtypeStruct((rows, width), bf16),
            jax.ShapeDtypeStruct((1, width), f32),
        ),
        in_specs=[vmem] * 5,
        out_specs=[pl.BlockSpec(memory_space=pl.ANY)] * 4,
        scratch_shapes=[
            pltpu.VMEM((rows, q_width), bf16),
            pltpu.VMEM((heads, rows), f32),
            dma((3 + kv_heads,)),
        ],
    )(*(pltpu.with_memory_space_constraint(part, pltpu.VMEM) for part in results))
    return (out[None], lse[None], rgrad[None], ggrad[0])


def solution(mesh):
    return jax.shard_map(
        functools.partial(per_device, mesh.shape["ctx"], mesh.shape["dp"]),
        mesh=mesh,
        in_specs=(
            P("dp", "ctx", None),
            P("dp", "ctx", None),
            P("dp", "ctx", None),
            P(),
            P("dp", "ctx", None),
            P("dp", "ctx", None),
            P(),
        ),
        out_specs=(P("dp", "ctx", None), P("dp", None, "ctx"), P("dp", "ctx", None), P()),
        check_vma=False,
    )
```

```python
import functools
import math

import jax
import jax.numpy as jnp
from jax import lax
from jax.experimental import pallas as pl
from jax.experimental.pallas import tpu as pltpu
from jax.sharding import PartitionSpec as P

HEAD_WIDTH = 128
MESH = pl.DeviceIdType.MESH
LOW = -1e30


def kernel(
    n,
    dp_count,
    heads,
    kv_heads,
    q_hbm,
    k_hbm,
    v_hbm,
    span_hbm,
    resid_hbm,
    grad_hbm,
    gain_hbm,
    summed,
    tops,
    totals,
    rgrad_buf,
    ggrad_buf,
    k_all,
    v_all,
    q_buf,
    q_turned,
    spans,
    resid_buf,
    grad_buf,
    gain_buf,
    terms,
    part,
    part_in,
    level,
    cross,
    whole,
    local_sem,
    kv_send,
    kv_recv,
    p1_send,
    p1_recv,
    p2_send,
    p2_recv,
    p3_send,
    p3_recv,
):
    rows = q_hbm.shape[0]
    width = resid_hbm.shape[1]
    span = rows // 2
    group = heads // kv_heads
    chips = n // 2
    piece = width // 2
    pair_heads = kv_heads // 2
    cut = pair_heads * HEAD_WIDTH
    me = lax.axis_index("ctx")
    mine_dp = lax.axis_index("dp")
    chip = me // 2
    core = me % 2
    sibling = chip * 2 + (1 - core)
    square = chips == 4

    def other_chip(k):
        if square:
            low, high = chip % 2, chip // 2
            low = 1 - low if k % 2 else low
            high = 1 - high if k // 2 else high
            return high * 2 + low
        return (chip + k) % chips

    def dp_peer(k):
        return (mine_dp + k) % dp_count

    barrier = pltpu.get_barrier_semaphore()
    pl.semaphore_signal(barrier, inc=1, device_id={"ctx": sibling}, device_id_type=MESH)
    for k in range(1, chips):
        peer = other_chip(k) * 2 + core
        pl.semaphore_signal(barrier, inc=1, device_id={"ctx": peer}, device_id_type=MESH)
    for k in range(1, dp_count):
        pl.semaphore_signal(barrier, inc=1, device_id={"dp": dp_peer(k)}, device_id_type=MESH)

    def slot(ref, index, count=1):
        return ref.at[pl.ds(pl.multiple_of(index * rows, rows), count * rows), :]

    own_k = pltpu.make_async_copy(k_hbm, slot(k_all, me), local_sem.at[0])
    own_v = pltpu.make_async_copy(v_hbm, slot(v_all, me), local_sem.at[1])
    get_resid = pltpu.make_async_copy(resid_hbm, resid_buf, local_sem.at[2])
    get_grad = pltpu.make_async_copy(grad_hbm, grad_buf, local_sem.at[3])
    get_gain = pltpu.make_async_copy(gain_hbm, gain_buf, local_sem.at[4])
    get_span = pltpu.make_async_copy(span_hbm, spans, local_sem.at[5])
    get_q = pltpu.make_async_copy(q_hbm, q_buf, local_sem.at[6])
    for copy in (own_k, own_v, get_resid, get_grad, get_gain, get_span, get_q):
        copy.start()

    k_or_v = (k_all, v_all)
    source = (k_hbm, v_hbm)
    sends = []

    def part_of(ref, half, index):
        at = pl.ds(pl.multiple_of(index * rows, rows), rows)
        return ref.at[at, half * cut : (half + 1) * cut]

    def carry(which, half, index, target, lane, first=False):
        held = part_of(k_or_v[which], half, index)
        return pltpu.make_async_remote_copy(
            src_ref=held,
            dst_ref=held,
            send_sem=kv_send.at[which, half, lane],
            recv_sem=kv_recv.at[which, half, index],
            device_id={"ctx": target},
            device_id_type=MESH,
        )

    def send(half, index, target, lane, first=False):
        for which in range(2):
            copy = carry(which, half, index, target, lane, first)
            copy.start()
            sends.append(copy)

    def arrived(half, index):
        for which in range(2):
            carry(which, half, index, sibling, 0).wait_recv()

    own_k.wait()
    own_v.wait()
    pl.semaphore_wait(barrier, chips + dp_count - 1)

    if square:
        send(0, me, other_chip(1) * 2 + core, 1, True)
        send(1, me, other_chip(2) * 2 + core, 2, True)
        send(1, me, other_chip(1) * 2 + core, 1, True)
        send(0, me, other_chip(2) * 2 + core, 2, True)
    else:
        for k in range(1, chips):
            for half in range(2):
                send(half, me, other_chip(k) * 2 + core, k, True)
    for half in range(2):
        send(half, me, sibling, 0, True)

    get_resid.wait()
    get_grad.wait()
    get_gain.wait()
    tile, cols = 16, 512
    terms[...] = jnp.zeros_like(terms)

    def norm_rows(step, carry):
        at = pl.ds(pl.multiple_of(step * tile, tile), tile)
        squares = jnp.zeros((tile, cols), jnp.float32)
        products = jnp.zeros((tile, cols), jnp.float32)
        for c in range(0, width, cols):
            r = resid_buf[at, c : c + cols].astype(jnp.float32)
            g = grad_buf[at, c : c + cols].astype(jnp.float32)
            squares = squares + r * r
            products = products + gain_buf[:, c : c + cols] * g * r
        mean_square = jnp.sum(squares, axis=1, keepdims=True) * (1.0 / width)
        inv = 1.0 / jnp.sqrt(mean_square + 1e-05)
        mean_product = jnp.sum(products, axis=1, keepdims=True) * inv * (1.0 / width)
        for c in range(0, width, cols):
            r = resid_buf[at, c : c + cols].astype(jnp.float32)
            g = grad_buf[at, c : c + cols].astype(jnp.float32)
            normed = r * inv
            term = g * normed
            terms[:, c : c + cols] += term[:8] + term[8:]
            scaled = gain_buf[:, c : c + cols] * g
            rgrad_buf[at, c : c + cols] = ((scaled - normed * mean_product) * inv).astype(
                rgrad_buf.dtype
            )
        return carry

    lax.fori_loop(0, rows // tile, norm_rows, 0)
    for r in range(2):
        part[r] = jnp.sum(terms[:, r * piece : (r + 1) * piece], axis=0, keepdims=True)

    join = pltpu.make_async_remote_copy(
        src_ref=part.at[1 - core],
        dst_ref=part_in.at[0],
        send_sem=p1_send.at[0],
        recv_sem=p1_recv.at[0],
        device_id={"ctx": sibling},
        device_id_type=MESH,
    )
    join.start()

    get_q.wait()
    for h in range(heads):
        turned = jnp.transpose(q_buf[:, h * HEAD_WIDTH : (h + 1) * HEAD_WIDTH])
        q_turned[h // group, :, (h % group) * rows : (h % group + 1) * rows] = turned

    join.wait()
    level[mine_dp] = part[core] + part_in[0]
    over_dp = []
    for k in range(1, dp_count):
        copy = pltpu.make_async_remote_copy(
            src_ref=level.at[mine_dp],
            dst_ref=level.at[mine_dp],
            send_sem=p2_send.at[k],
            recv_sem=p2_recv.at[k],
            device_id={"dp": dp_peer(k)},
            device_id_type=MESH,
        )
        copy.start()
        over_dp.append(copy)

    get_span.wait()
    lane = lax.broadcasted_iota(jnp.int32, (1, rows), 1)
    q_pos = (
        jnp.where(lane < span, spans[2 * me], spans[2 * me + 1]) * span + lane % span
    )
    scale = HEAD_WIDTH ** (-0.5)
    exponent = scale * math.log2(math.e)

    def fold(index, count, half, first=False):
        line = lax.broadcasted_iota(jnp.int32, (count * rows, 1), 0)
        base = jnp.full((count * rows, 1), spans[2 * index], jnp.int32)
        for i in range(1, 2 * count):
            base = jnp.where(line >= i * span, spans[2 * index + i], base)
        k_pos = base * span + line % span
        bias = jnp.where(k_pos <= q_pos, 0.0, LOW)
        at = pl.ds(pl.multiple_of(index * rows, rows), count * rows)
        products = [
            jnp.dot(
                k_all[at, h * HEAD_WIDTH : (h + 1) * HEAD_WIDTH],
                q_turned[h],
                preferred_element_type=jnp.float32,
            )
            for h in range(half * pair_heads, (half + 1) * pair_heads)
        ]
        for h in range(half * pair_heads, (half + 1) * pair_heads):
            band = slice(h * HEAD_WIDTH, (h + 1) * HEAD_WIDTH)
            scores = products[h - half * pair_heads]
            probs, factors = [], []
            for g in range(group):
                lanes = slice(g * rows, (g + 1) * rows)
                s = scores[:, lanes] + bias
                top = jnp.max(s, axis=0, keepdims=True)
                if not first:
                    before = tops[h : h + 1, lanes]
                    top = jnp.maximum(top, before)
                    factor = jnp.exp2((before - top) * exponent)
                    factors.append(factor)
                w = jnp.exp2((s - top) * exponent)
                total = jnp.sum(w, axis=0, keepdims=True)
                if not first:
                    total = total + totals[h : h + 1, lanes] * factor
                tops[h : h + 1, lanes] = top
                totals[h : h + 1, lanes] = total
                probs.append(w.astype(jnp.bfloat16))
            added = lax.dot_general(
                v_all[at, band],
                jnp.concatenate(probs, axis=1),
                (((0,), (0,)), ((), ())),
                preferred_element_type=jnp.float32,
            )
            if first:
                summed[h] = added
            else:
                summed[h] = summed[h] * jnp.concatenate(factors, axis=1) + added

    for half in range(2):
        arrived(half, sibling)
        fold(chip * 2, 2, half, True)

    def gain_chips():
        for copy in over_dp:
            copy.wait()
        cross[chip] = jnp.sum(level[...], axis=0)
        copies = []
        for k in range(1, chips):
            copy = pltpu.make_async_remote_copy(
                src_ref=cross.at[chip],
                dst_ref=cross.at[chip],
                send_sem=p3_send.at[k],
                recv_sem=p3_recv.at[k],
                device_id={"ctx": other_chip(k) * 2 + core},
                device_id_type=MESH,
            )
            copy.start()
            copies.append(copy)
        return copies

    def gain_whole(copies):
        for copy in copies:
            copy.wait()
        whole[core] = jnp.sum(cross[...], axis=0)
        copy = pltpu.make_async_remote_copy(
            src_ref=whole.at[core],
            dst_ref=whole.at[core],
            send_sem=p1_send.at[1],
            recv_sem=p1_recv.at[1],
            device_id={"ctx": sibling},
            device_id_type=MESH,
        )
        copy.start()
        return copy

    if square:
        near, far, across = other_chip(1), other_chip(2), other_chip(3)
        near_c, far_c, across_c = near * 2 + core, far * 2 + core, across * 2 + core
        arrived(0, near_c)
        send(0, near_c, far_c, 3)
        send(0, near_c, sibling, 4)
        arrived(1, far_c)
        send(1, far_c, near_c, 3)
        send(1, far_c, sibling, 4)
        over_chips = gain_chips()
        arrived(0, near * 2 + 1 - core)
        fold(near * 2, 2, 0)
        arrived(1, far * 2 + 1 - core)
        fold(far * 2, 2, 1)
        arrived(1, near_c)
        send(1, near_c, sibling, 5)
        arrived(0, far_c)
        send(0, far_c, sibling, 5)
        fold(near_c, 1, 1)
        fold(far_c, 1, 0)
        arrived(1, near * 2 + 1 - core)
        fold(near * 2 + 1 - core, 1, 1)
        arrived(0, far * 2 + 1 - core)
        fold(far * 2 + 1 - core, 1, 0)
        for half in range(2):
            arrived(half, across_c)
            send(half, across_c, sibling, 6)
        for half in range(2):
            fold(across_c, 1, half)
        last = gain_whole(over_chips)
        for half in range(2):
            arrived(half, across * 2 + 1 - core)
            fold(across * 2 + 1 - core, 1, half)
    else:
        over_chips = gain_chips()

        def step(k, unused):
            other = (chip + chips - k) % chips
            held = other * 2 + core
            copies = []
            for half in range(2):
                arrived(half, held)
                for which in range(2):
                    copy = carry(which, half, held, sibling, chips)
                    copy.start()
                    copies.append(copy)
            for half in range(2):
                arrived(half, other * 2 + 1 - core)
                fold(other * 2, 2, half)
            for copy in copies:
                copy.wait_send()
            return unused

        lax.fori_loop(1, chips, step, 0)
        last = gain_whole(over_chips)

    last.wait()
    for r in range(2):
        ggrad_buf[:, r * piece : (r + 1) * piece] = whole[r]
    for copy in sends:
        copy.wait_send()

def finish(
    heads, kv_heads, summed, tops, totals, rgrad, ggrad,
    out_hbm, lse_hbm, rgrad_hbm, ggrad_hbm, out_buf, lse_buf, sem
):
    rows = out_hbm.shape[0]
    group = heads // kv_heads
    scale = HEAD_WIDTH ** (-0.5)
    puts = [
        pltpu.make_async_copy(rgrad, rgrad_hbm, sem.at[0]),
        pltpu.make_async_copy(ggrad, ggrad_hbm, sem.at[1]),
    ]
    for copy in puts:
        copy.start()
    for kv in range(kv_heads):
        for g in range(group):
            h = kv * group + g
            lanes = slice(g * rows, (g + 1) * rows)
            total = totals[kv : kv + 1, lanes]
            lse_buf[h : h + 1, :] = tops[kv : kv + 1, lanes] * scale + jnp.log(total)
            out_buf[:, h * HEAD_WIDTH : (h + 1) * HEAD_WIDTH] = jnp.transpose(
                summed[kv, :, lanes] * (1.0 / total)
            ).astype(out_buf.dtype)
        band = pl.ds(kv * group * HEAD_WIDTH, group * HEAD_WIDTH)
        copy = pltpu.make_async_copy(out_buf.at[:, band], out_hbm.at[:, band], sem.at[3 + kv])
        copy.start()
        puts.append(copy)
    copy = pltpu.make_async_copy(lse_buf, lse_hbm, sem.at[2])
    copy.start()
    puts.append(copy)
    for copy in puts:
        copy.wait()


def per_device(n, dp_count, query, key, value, span_order, resid, grad_norm, gain):
    rows, q_width = query.shape[1:]
    kv_width = key.shape[2]
    width = resid.shape[2]
    heads, kv_heads = q_width // HEAD_WIDTH, kv_width // HEAD_WIDTH
    group = heads // kv_heads
    piece = width // 2
    f32, bf16 = jnp.float32, jnp.bfloat16
    dma = pltpu.SemaphoreType.DMA
    lanes = max(8, n // 2 + 1)
    middle = (
        pltpu.VMEM((kv_heads, HEAD_WIDTH, group * rows), f32),
        pltpu.VMEM((kv_heads, group * rows), f32),
        pltpu.VMEM((kv_heads, group * rows), f32),
        pltpu.VMEM((rows, width), bf16),
        pltpu.VMEM((1, width), f32),
    )
    vmem = pl.BlockSpec(memory_space=pltpu.VMEM)
    results = pl.pallas_call(
        functools.partial(kernel, n, dp_count, heads, kv_heads),
        out_shape=middle,
        in_specs=[pl.BlockSpec(memory_space=pl.ANY)] * 7,
        out_specs=[vmem] * 5,
        scratch_shapes=[
            pltpu.VMEM((n * rows, kv_width), bf16),
            pltpu.VMEM((n * rows, kv_width), bf16),
            pltpu.VMEM((rows, q_width), bf16),
            pltpu.VMEM((kv_heads, HEAD_WIDTH, group * rows), bf16),
            pltpu.SMEM(span_order.shape, jnp.int32),
            pltpu.VMEM((rows, width), bf16),
            pltpu.VMEM((rows, width), bf16),
            pltpu.VMEM((1, width), f32),
            pltpu.VMEM((8, width), f32),
            pltpu.VMEM((2, 1, piece), f32),
            pltpu.VMEM((1, 1, piece), f32),
            pltpu.VMEM((dp_count, 1, piece), f32),
            pltpu.VMEM((n // 2, 1, piece), f32),
            pltpu.VMEM((2, 1, piece), f32),
            dma((7,)),
            dma((2, 2, lanes)),
            dma((2, 2, n)),
            dma((2,)),
            dma((2,)),
            dma((dp_count,)),
            dma((dp_count,)),
            dma((n // 2,)),
            dma((n // 2,)),
        ],
        compiler_params=pltpu.CompilerParams(collective_id=0, has_side_effects=True),
    )(
        query[0],
        key[0],
        value[0],
        span_order,
        resid[0],
        grad_norm[0],
        gain[None, :],
    )
    out, lse, rgrad, ggrad = pl.pallas_call(
        functools.partial(finish, heads, kv_heads),
        out_shape=(
            jax.ShapeDtypeStruct((rows, q_width), bf16),
            jax.ShapeDtypeStruct((heads, rows), f32),
            jax.ShapeDtypeStruct((rows, width), bf16),
            jax.ShapeDtypeStruct((1, width), f32),
        ),
        in_specs=[vmem] * 5,
        out_specs=[pl.BlockSpec(memory_space=pl.ANY)] * 4,
        scratch_shapes=[
            pltpu.VMEM((rows, q_width), bf16),
            pltpu.VMEM((heads, rows), f32),
            dma((3 + kv_heads,)),
        ],
    )(*(pltpu.with_memory_space_constraint(part, pltpu.VMEM) for part in results))
    return (out[None], lse[None], rgrad[None], ggrad[0])


def solution(mesh):
    return jax.shard_map(
        functools.partial(per_device, mesh.shape["ctx"], mesh.shape["dp"]),
        mesh=mesh,
        in_specs=(
            P("dp", "ctx", None),
            P("dp", "ctx", None),
            P("dp", "ctx", None),
            P(),
            P("dp", "ctx", None),
            P("dp", "ctx", None),
            P(),
        ),
        out_specs=(P("dp", "ctx", None), P("dp", None, "ctx"), P("dp", "ctx", None), P()),
        check_vma=False,
    )
```
